256 devices in a mesh: rep: 32 (over x, z_lo, y), shard: 8 (over z_hi, core).
Axes of the slice: x: 4, y: 4, z: 8 (z_hi: 4, z_lo: 2; z = z_hi * 2 + z_lo), core: 2. Of those that a mesh axis runs over, the one named last changes fastest.
Arguments:
- params: float32 [32, 1600, 3200], P('rep', None, 'shard'), may hold values from -6 to 6
- momentum: float32 [32, 1600, 3200], P('rep', None, 'shard'), may hold values from -6 to 6
- tokens: bfloat16 [32, 2, 1024, 1600], P('rep', None, 'shard'), may hold values from -6 to 6
- targets: bfloat16 [32, 2, 1024, 3200], P('rep', None, None, 'shard'), may hold values from -6 to 6
- blend_weight: float32 [3200], P('shard'), may hold values from 0.2 to 0.9
Outputs:
- averaged: float32 [1600, 3200], P(None, 'shard')
- blended: float32 [32, 1600, 3200], P('rep', None, 'shard')
The draws below stay inside these ranges and needn't reach their ends.
All inputs are finite; a program needn't handle non-finite values.
Results may differ from the reference program's by a relative error of at most 0.0045.
Values may be sent and summed in bfloat16 or wider, within the bound.
No kernel may reach another device: no remote copies, remote signals or barrier semaphores. Data moves between devices by JAX's collectives and lax.ppermute only.
A program may use at most 128 MiB of HBM per device.

```python
import math
import jax
import jax.numpy as jnp
from jax import lax

D = 1600
FFW = 3200
H = 2
TOKS = 1024
REPS = 32


def levels(stream_key, extent, cuts, low, largest):
    def one(position, blocks):
        steps = jax.random.uniform(jax.random.fold_in(jax.random.fold_in(stream_key, 6), position), (blocks,), jnp.float32, low / len(cuts), largest / len(cuts))
        return jnp.repeat(jnp.exp(steps), extent[position] // blocks).reshape((-1,) + (1,) * (len(extent) - position - 1))

    gain = one(*cuts[0])
    for cut in cuts[1:]:
        gain = gain * one(*cut)
    return gain


def scatter_about(stream_key, shape, width, reach, shards=(), dtype=jnp.bfloat16):
    values = width * jax.random.normal(stream_key, shape, jnp.float32)
    if shards:
        values = values * levels(stream_key, shape, shards, -0.22, 0.18)
    return jnp.clip(values, -reach, reach).astype(dtype)


def setup_inputs(seed: int = 0) -> dict:
    arg_keys = jax.random.split(jax.random.key(seed), 6)
    params = scatter_about(arg_keys[0], (REPS, D, FFW), 1.0, 6.0, ((0, 32), (2, 8)), jnp.float32)
    momentum = scatter_about(arg_keys[1], (REPS, D, FFW), 1.0, 6.0, ((0, 32), (2, 8)), jnp.float32)
    tokens = scatter_about(arg_keys[2], (REPS, H, TOKS, D), 1.0, 6.0, ((0, 32), (2, 8)))
    targets = scatter_about(arg_keys[3], (REPS, H, TOKS, FFW), 1.0, 6.0, ((0, 32), (3, 8)))
    blend_weight = jnp.clip(jnp.exp(math.log(0.9) - 1.50407736 * jax.random.uniform(arg_keys[4], (FFW,), jnp.float32) ** levels(arg_keys[4], (FFW,), ((0, 8),), -0.2, 0.2)), 0.2, 0.9)
    return {"params": params, "momentum": momentum, "tokens": tokens, "targets": targets, "blend_weight": blend_weight}


learn_rate = 0.05
momentum_decay = 0.9

def gelu_tanh(value):
    return jax.nn.gelu(value, approximate=True)

def replica(weight, moment, inputs, wanted):
    scaling = 1.0 / jnp.sqrt(jnp.float32(D))
    for local_step in range(H):
        weight_half = weight.astype(jnp.bfloat16)
        pre = jnp.dot(inputs[local_step], weight_half, preferred_element_type=jnp.float32) * scaling
        activation, pullback = jax.vjp(gelu_tanh, pre)
        slope, = pullback(activation - wanted[local_step].astype(jnp.float32))
        hidden_grad = (slope * scaling).astype(jnp.bfloat16)
        gradient = lax.dot_general(inputs[local_step], hidden_grad, (((0,), (0,)), ((), ())), preferred_element_type=jnp.float32)
        moment = momentum_decay * moment + gradient
        weight = weight - learn_rate * moment
    return (weight, moment)

def reference(params, momentum, tokens, targets, blend_weight):
    weights, moments = lax.map(lambda packed: replica(*packed), (params, momentum, tokens, targets))
    averaged = lax.optimization_barrier(jnp.sum(weights, axis=0)) / jnp.float32(REPS)
    mean_moment = lax.optimization_barrier(jnp.sum(moments, axis=0)) / jnp.float32(REPS)
    blended = blend_weight * mean_moment[None] + (1.0 - blend_weight) * moments
    return (averaged, blended)
```

```python
import math

import jax
import jax.numpy as jnp
from jax import lax
from jax.experimental import pallas as pl
from jax.experimental.pallas import tpu as pltpu
from jax.sharding import PartitionSpec as P

D = 1600
TOP = D // 2
LANES = 128
SCALE = 1.0 / math.sqrt(D)
LEARN = 0.05
DECAY = 0.9


def rotated(up, cores):
    return [(2 * z + c, 2 * ((z + up) % 4) + (c + cores) % 2) for z in range(4) for c in range(2)]


def slope(pre, wanted):
    k = math.sqrt(2.0 / math.pi)
    square = pre * pre
    th = jnp.tanh(k * (pre + 0.044715 * pre * square))
    half = 0.5 * (1.0 + th)
    deriv = half + 0.5 * pre * (1.0 - th * th) * (k * (1.0 + 3 * 0.044715 * square))
    return (pre * half - wanted) * deriv * SCALE


def partial_gradient(at, weight, wanted, blocks, x):
    for i, (top, bottom) in enumerate(blocks):
        x[:TOP, i * LANES : (i + 1) * LANES] = top[...]
        x[TOP:, i * LANES : (i + 1) * LANES] = bottom[...]
    pre = jnp.dot(weight, x[...], preferred_element_type=jnp.float32) * SCALE
    want = jnp.concatenate(
        [wanted[:, pl.ds(pl.multiple_of(at[i] * LANES, LANES), LANES)] for i in range(len(blocks))], axis=1
    )
    hidden = slope(pre, want.astype(jnp.float32)).astype(jnp.bfloat16)
    return lax.dot_general(hidden, x[...], (((1,), (1,)), ((), ())), preferred_element_type=jnp.float32)


def pairs(refs):
    return [(refs[i], refs[i + 1]) for i in range(0, len(refs), 2)]


def early_kernel(at, weight, wanted, *refs):
    *blocks, out, x = refs
    out[...] = partial_gradient(at, weight[...].astype(jnp.bfloat16), wanted, pairs(blocks), x)


def pack(lines, value):
    units = value.shape[0]
    full = D // LANES
    for j in range(full):
        lines[j * units : (j + 1) * units, :] = value[:, j * LANES : (j + 1) * LANES].astype(jnp.bfloat16)
    rest = value[:, full * LANES :]
    at = full * units
    folded = jnp.concatenate([rest[: units // 2], rest[units // 2 :]], axis=1)
    lines[at : at + units // 2, :] = folded.astype(jnp.bfloat16)
    at += units // 2
    lines[at:, :] = jnp.zeros((lines.shape[0] - at, LANES), jnp.bfloat16)


def late_first_kernel(at, weight, wanted, grad, moment, *refs):
    *blocks, moment_out, weight_out, lines, x = refs
    g = partial_gradient(at, weight[...].astype(jnp.bfloat16), wanted, pairs(blocks), x)
    m = DECAY * moment[...] + (grad[...] + g)
    moment_out[...] = m
    w = weight[...] - LEARN * m
    weight_out[...] = w.astype(jnp.bfloat16)
    pack(lines, w)


def late_second_kernel(at, weight, wanted, grad, moment, *refs):
    *blocks, moment_out, lines, x = refs
    g = partial_gradient(at, weight[...], wanted, pairs(blocks), x)
    m = DECAY * moment[...] + (grad[...] + g)
    moment_out[...] = m
    pack(lines, m)


def last_kernel(blend, mean_weight, mean_moment, moment, averaged, blended):
    units = moment.shape[0]
    b = blend[...]

    def put(lanes, w, m):
        m = m.astype(jnp.float32)
        averaged[:, lanes] = w.astype(jnp.float32) - LEARN * m
        blended[:, lanes] = b * m + (1.0 - b) * moment[:, lanes]

    full = D // LANES
    for j in range(full):
        rows = slice(j * units, (j + 1) * units)
        put(slice(j * LANES, (j + 1) * LANES), mean_weight[rows, :], mean_moment[rows, :])
    rows = slice(full * units, full * units + units // 2)

    def unfold(v):
        v = v.astype(jnp.float32)
        half = LANES // 2
        return jnp.concatenate([v[:, :half], v[:, half:]], axis=0)

    put(slice(full * LANES, D), unfold(mean_weight[rows, :]), unfold(mean_moment[rows, :]))


SMEM = pl.BlockSpec(memory_space=pltpu.SMEM)
VMEM = pl.BlockSpec(memory_space=pltpu.VMEM)


def cost(tokens, units):
    return pl.CostEstimate(flops=4 * tokens * units * D, bytes_accessed=8 * units * D, transcendentals=tokens * units)


def call(kernel, outs, args, blocks, name):
    tokens = LANES * len(blocks) // 2
    return pl.pallas_call(
        kernel,
        out_shape=outs,
        in_specs=[SMEM] + [VMEM] * (len(args) - 1 + len(blocks)),
        out_specs=jax.tree.map(lambda _: VMEM, outs),
        scratch_shapes=[pltpu.VMEM((D, tokens), jnp.bfloat16)],
        cost_estimate=cost(tokens, args[1].shape[0]),
        name=name,
    )(*args, *blocks)


def shard_permute(v, up, cores):
    return lax.ppermute(v, "shard", rotated(up, cores))


def gather(piece):
    top, bottom = piece
    low_top = shard_permute(top, 1, 0)
    high_bottom = shard_permute(bottom, -1, 0)
    low_bottom = shard_permute(bottom, 1, 0)
    high_top = shard_permute(top, -1, 0)
    far_top = shard_permute(low_top, 1, 0)
    far_bottom = shard_permute(high_bottom, -1, 0)
    near = [top, bottom, low_top, low_bottom, high_top, high_bottom]
    return near, [far_top, far_bottom], (low_bottom, high_top)


def other_core(values):
    return [shard_permute(v, 0, 1) for v in values]


def scattered_mean(lines, axis):
    count = lax.axis_size(axis)
    got = lax.all_to_all(lines.reshape(count, -1, LANES), axis, 0, 0)
    return (jnp.sum(got.astype(jnp.float32), axis=0) / count).astype(jnp.bfloat16)


def gathered(mean, axis):
    count = lax.axis_size(axis)
    return lax.all_to_all(jnp.broadcast_to(mean[None], (count, *mean.shape)), axis, 0, 0).reshape(-1, LANES)


def local(params, momentum, tokens, targets, blend_weight):
    weight = params[0].T
    moment = momentum[0].T
    units = weight.shape[0]
    pieces = jnp.swapaxes(tokens[0], 1, 2)
    wanted = jnp.swapaxes(targets[0], 1, 2)
    me = lax.axis_index("shard")
    z, c = me // 2, me % 2
    near_at = jnp.stack([2 * ((z + up) % 4) + (c + k) % 2 for k in range(2) for up in (0, -1, 1)])
    far_at = jnp.stack([2 * ((z + 2) % 4) + (c + k) % 2 for k in range(2)])
    replicas = lax.axis_size("rep")
    rows = -(-units * D // (LANES * 8 * replicas)) * 8 * replicas

    whole = jax.ShapeDtypeStruct((units, D), jnp.float32)
    half = jax.ShapeDtypeStruct((units, D), jnp.bfloat16)
    lines = jax.ShapeDtypeStruct((rows, LANES), jnp.bfloat16)

    first = pieces[0, :TOP], pieces[0, TOP:]
    second = pieces[1, :TOP], pieces[1, TOP:]
    near, far, sent = gather(first)
    second, _ = lax.optimization_barrier((second, sent))
    near2, far2, _ = gather(second)

    near += other_core(near)
    far += other_core(far)
    grad = call(early_kernel, whole, (near_at, weight, wanted[0]), near, "early_first")
    moment, weight, weight_lines = call(
        late_first_kernel, (whole, half, lines), (far_at, weight, wanted[0], grad, moment), far, "late_first"
    )
    mean_weight = gathered(scattered_mean(weight_lines, "rep"), "rep")

    near2 += other_core(near2)
    far2 += other_core(far2)
    grad = call(early_kernel, whole, (near_at, weight, wanted[1]), near2, "early_second")
    moment, moment_lines = call(
        late_second_kernel, (whole, lines), (far_at, weight, wanted[1], grad, moment), far2, "late_second"
    )
    mean_moment = gathered(scattered_mean(moment_lines, "rep"), "rep")
    averaged, blended = pl.pallas_call(
        last_kernel,
        out_shape=(whole, whole),
        in_specs=[VMEM] * 4,
        out_specs=(VMEM, VMEM),
        name="last",
    )(blend_weight[:, None], mean_weight, mean_moment, moment)
    return averaged.T, blended.T[None]


def solution(mesh):
    return jax.shard_map(
        local,
        mesh=mesh,
        in_specs=(
            P("rep", None, "shard"),
            P("rep", None, "shard"),
            P("rep", None, "shard", None),
            P("rep", None, None, "shard"),
            P("shard"),
        ),
        out_specs=(P(None, "shard"), P("rep", None, "shard")),
        check_vma=False,
    )
```

```python
import math

import jax
import jax.numpy as jnp
from jax import lax
from jax.experimental import pallas as pl
from jax.experimental.pallas import tpu as pltpu
from jax.sharding import PartitionSpec as P


D = 1600
TOP = D // 2
LANES = 128
SCALE = 1.0 / math.sqrt(D)
LEARN = 0.05
DECAY = 0.9


def rotated(up, cores):
    return [(2 * z + c, 2 * ((z + up) % 4) + (c + cores) % 2) for z in range(4) for c in range(2)]


def slope(pre, wanted):
    k = math.sqrt(2.0 / math.pi)
    square = pre * pre
    th = jnp.tanh(k * (pre + 0.044715 * pre * square))
    half = 0.5 * (1.0 + th)
    deriv = half + 0.5 * pre * (1.0 - th * th) * (k * (1.0 + 3 * 0.044715 * square))
    return (pre * half - wanted) * deriv * SCALE


def places(me, ups):
    z, c = me // 2, me % 2
    return [2 * ((z + up) % 4) + (c + k) % 2 for k in range(2) for up in ups]


def partial_gradient(step, at, weight, wanted, blocks, x):
    for i, (top, bottom) in enumerate(blocks):
        x[:TOP, i * LANES : (i + 1) * LANES] = top[...]
        x[TOP:, i * LANES : (i + 1) * LANES] = bottom[...]
    pre = jnp.dot(weight, x[...], preferred_element_type=jnp.float32) * SCALE
    want = jnp.concatenate(
        [wanted[step, :, pl.ds(pl.multiple_of(a * LANES, LANES), LANES)] for a in at], axis=1
    )
    hidden = slope(pre, want.astype(jnp.float32)).astype(jnp.bfloat16)
    return lax.dot_general(hidden, x[...], (((1,), (1,)), ((), ())), preferred_element_type=jnp.float32)


def pairs(refs):
    return [(refs[i], refs[i + 1]) for i in range(0, len(refs), 2)]


def early_kernel(step):
    def kernel(me, weight, wanted, *refs):
        *blocks, out, x = refs
        at = places(me[0], (0, 3, 1))
        out[...] = partial_gradient(step, at, weight[...].astype(jnp.bfloat16), wanted, pairs(blocks), x)

    return kernel


UNITS = 80
LINES = 1024
FULL = D // LANES


def pack(lines, value):
    for j in range(FULL):
        lines[j * UNITS : (j + 1) * UNITS, :] = value[:, j * LANES : (j + 1) * LANES].astype(jnp.bfloat16)
    rest = value[:, FULL * LANES :]
    folded = jnp.concatenate([rest[: UNITS // 2], rest[UNITS // 2 :]], axis=1)
    at = FULL * UNITS
    lines[at : at + UNITS // 2, :] = folded.astype(jnp.bfloat16)
    at += UNITS // 2
    lines[at:, :] = jnp.zeros((LINES - at, LANES), jnp.bfloat16)


def unpacked(lines, at):
    for j in range(FULL):
        yield slice(j * LANES, (j + 1) * LANES), lines[pl.ds(at + j * UNITS, UNITS), :].astype(jnp.float32)
    rest = lines[pl.ds(at + FULL * UNITS, UNITS // 2), :].astype(jnp.float32)
    half = LANES // 2
    yield slice(FULL * LANES, D), jnp.concatenate([rest[:, :half], rest[:, half:]], axis=0)


def late_kernel(step):
    def kernel(me, weight, wanted, grad, moment, *refs):
        count = 3 if step == 0 else 2
        blocks, refs = refs[:4], refs[4:]
        outs, bufs, (x, g, done) = refs[:count], refs[count : 2 * count], refs[2 * count :]
        at = places(me[0], (2,))
        g[...] = partial_gradient(step, at, weight[...].astype(jnp.bfloat16), wanted, pairs(blocks), x)
        copies = []
        for i in range(weight.shape[0] // UNITS):
            rows = slice(i * UNITS, (i + 1) * UNITS)
            taken = [slice(i * LINES, (i + 1) * LINES), rows, rows][:count]
            m = DECAY * moment[rows, :] + (grad[rows, :] + g[rows, :])
            bufs[1][rows, :] = m
            if step == 0:
                m = weight[rows, :] - LEARN * m
                bufs[2][rows, :] = m.astype(jnp.bfloat16)
            pack(bufs[0].at[taken[0], :], m)
            for k in range(count):
                copy = pltpu.make_async_copy(bufs[k].at[taken[k], :], outs[k].at[taken[k], :], done.at[k, i])
                copy.start()
                copies.append(copy)
        for copy in copies:
            copy.wait()

    return kernel


def last_kernel(blend, lines, mean_weight, moment, averaged, blended):
    b = blend[...]
    for lanes, m in unpacked(lines, pl.multiple_of(pl.program_id(0) * LINES, LINES)):
        averaged[:, lanes] = mean_weight[:, lanes].astype(jnp.float32) - LEARN * m
        blended[:, lanes] = b * m + (1.0 - b) * moment[:, lanes]


ROUND = (0, 3, 1, 2)


def spread_kernel(me, *refs):
    *parts, out, lines = refs
    x, y, core = me[0] // 8, me[0] % 4, me[1] % 2
    rows = lines.shape[0] // 16
    for part, far in zip(parts, ROUND):
        for i, near in enumerate(ROUND):
            dx, dy = near + core * (far - near), far + core * (near - far)
            owner = (x + dy) % 4 * 4 + (y + dx) % 4
            lines[pl.ds(pl.multiple_of(owner * rows, rows), rows), :] = part[i * rows : (i + 1) * rows, :]
    for u in range(out.shape[0] // UNITS):
        for lanes, v in unpacked(lines, u * LINES):
            out[u * UNITS : (u + 1) * UNITS, lanes] = v.astype(jnp.bfloat16)


SMEM = pl.BlockSpec(memory_space=pltpu.SMEM)
VMEM = pl.BlockSpec(memory_space=pltpu.VMEM)
MIB = 1 << 20


def call(kernel, outs, args, blocks, late):
    tokens, units = LANES * len(blocks) // 2, args[1].shape[0]
    scratch = [pltpu.VMEM((D, tokens), jnp.bfloat16)]
    if late:
        scratch = [pltpu.VMEM(o.shape, o.dtype) for o in outs] + scratch + [pltpu.VMEM((units, D), jnp.float32)]
        scratch.append(pltpu.SemaphoreType.DMA((len(outs), units // UNITS)))
    return pl.pallas_call(
        kernel,
        out_shape=tuple(pltpu.HBM(o.shape, o.dtype) for o in outs) if late else outs,
        in_specs=[SMEM] + [VMEM] * (len(args) - 1 + len(blocks)),
        out_specs=(pl.BlockSpec(memory_space=pltpu.HBM),) * len(outs) if late else VMEM,
        scratch_shapes=scratch,
        cost_estimate=pl.CostEstimate(
            flops=4 * tokens * units * D, bytes_accessed=8 * units * D, transcendentals=tokens * units
        ),
        compiler_params=pltpu.CompilerParams(vmem_limit_bytes=24 * MIB),
    )(*args, *blocks)


def gate_kernel(me, out):
    out[0] = me[0]


def gate(me):
    return pl.pallas_call(
        gate_kernel,
        out_shape=jax.ShapeDtypeStruct((1,), jnp.int32),
        in_specs=[SMEM],
        out_specs=SMEM,
        compiler_params=pltpu.CompilerParams(vmem_limit_bytes=MIB),
    )(me)


def shard_permute(v, up, cores):
    return lax.ppermute(v, "shard", rotated(up, cores))


def gather(piece):
    top, bottom = piece
    low_top = shard_permute(top, 1, 0)
    high_bottom = shard_permute(bottom, -1, 0)
    low_bottom = shard_permute(bottom, 1, 0)
    high_top = shard_permute(top, -1, 0)
    far_top = shard_permute(low_top, 1, 0)
    far_bottom = shard_permute(high_bottom, -1, 0)
    near = [top, bottom, low_top, low_bottom, high_top, high_bottom]
    return near, [far_top, far_bottom], (low_top, high_bottom)


def other_core(values):
    return [shard_permute(v, 0, 1) for v in values]


def added(got):
    return jnp.sum(got[...].astype(jnp.float32), axis=0)


def sum_kernel(got, out):
    out[...] = added(got).astype(jnp.bfloat16)


def mean_kernel(got, out):
    mean = (added(got) / got.shape[0]).astype(jnp.bfloat16)
    out[...] = jnp.broadcast_to(mean[None], out.shape)


def pair_kernel(here, there, out):
    out[...] = ((here[...].astype(jnp.float32) + there[...].astype(jnp.float32)) / 32).astype(jnp.bfloat16)


def small(kernel, args, shape):
    return pl.pallas_call(
        kernel,
        out_shape=jax.ShapeDtypeStruct(shape, jnp.bfloat16),
        in_specs=[VMEM] * len(args),
        out_specs=VMEM,
        compiler_params=pltpu.CompilerParams(vmem_limit_bytes=8 * MIB),
    )(*args)


def join_kernel(*refs):
    *parts, out = refs
    at = 0
    for part in parts:
        out[at : at + part.shape[0], :] = part[...]
        at += part.shape[0]


def replica_permute(v, core0, core1):
    pairs = []
    for r in range(32):
        for k in range(8):
            x, z, y = (core0, core1)[k % 2]
            to = 8 * ((r // 8 + x) % 4) + 4 * ((r // 4 + z) % 2) + (r + y) % 4
            pairs.append((8 * r + k, 8 * to + k))
    return lax.ppermute(v, ("rep", "shard"), pairs)


def weight_mean(lines):
    planes = [[8 * x + 4 * z + y for x in range(4) for y in range(4)] for z in range(2)]
    got = lax.all_to_all(lines.reshape(16, -1, LANES), "rep", 0, 0, axis_index_groups=planes)
    part = got.shape[1:]
    here = small(sum_kernel, [got], part)
    there = replica_permute(here, (0, 1, 0), (0, 1, 0))
    chunk = small(pair_kernel, [here, there], part)
    line = [replica_permute(chunk, (0, 0, k), (k, 0, 0)) for k in (1, 3, 2)]
    plane = small(join_kernel, [chunk, *line], (4 * part[0], LANES))
    return [plane] + [replica_permute(plane, (k, 0, 0), (0, 0, k)) for k in (1, 3, 2)]


def body(params, momentum, tokens, targets, blend_weight):
    weight = params[0].T
    moment = momentum[0].T
    units = weight.shape[0]
    pieces = jnp.swapaxes(tokens[0], 1, 2)
    wanted = jnp.swapaxes(targets[0], 1, 2)
    me = lax.axis_index("shard")[None]
    replicas = lax.axis_size("rep")
    rows = units // UNITS * LINES

    whole = jax.ShapeDtypeStruct((units, D), jnp.float32)
    half = jax.ShapeDtypeStruct((units, D), jnp.bfloat16)
    lines = jax.ShapeDtypeStruct((rows, LANES), jnp.bfloat16)

    first = pieces[0, :TOP], pieces[0, TOP:]
    second = pieces[1, :TOP], pieces[1, TOP:]
    near, far, sent = gather(first)
    second, _ = lax.optimization_barrier((second, sent))
    near2, far2, _ = gather(second)

    near += other_core(near)
    far += other_core(far)
    grad = call(early_kernel(0), whole, (gate(me), weight, wanted), near, False)
    weight_lines, moment, weight = call(
        late_kernel(0), (lines, whole, half), (me, weight, wanted, grad, moment), far, True
    )
    parts = weight_mean(weight_lines)

    near2 += other_core(near2)
    far2 += other_core(far2)
    grad = call(early_kernel(1), whole, (gate(me), weight, wanted), near2, False)
    moment_lines, moment = call(late_kernel(1), (lines, whole), (me, weight, wanted, grad, moment), far2, True)
    got = lax.all_to_all(moment_lines.reshape(replicas, -1, LANES), "rep", 0, 0)
    means = small(mean_kernel, [got], got.shape)
    mean_moment = lax.all_to_all(means, "rep", 0, 0).reshape(-1, LANES)

    mean_weight = pl.pallas_call(
        spread_kernel,
        out_shape=half,
        in_specs=[SMEM] + [VMEM] * 4,
        out_specs=VMEM,
        scratch_shapes=[pltpu.VMEM((rows, LANES), jnp.bfloat16)],
        compiler_params=pltpu.CompilerParams(vmem_limit_bytes=12 * MIB),
        name="spread",
    )(jnp.stack([lax.axis_index("rep"), lax.axis_index("shard")]), *parts)
    block = pl.BlockSpec((UNITS, D), lambda i: (i, 0))
    averaged, blended = pl.pallas_call(
        last_kernel,
        grid=(units // UNITS,),
        out_shape=(whole, whole),
        in_specs=[pl.BlockSpec((UNITS, 1), lambda i: (i, 0)), VMEM, block, block],
        out_specs=(block, block),
        compiler_params=pltpu.CompilerParams(vmem_limit_bytes=12 * MIB),
        name="last",
    )(blend_weight[:, None], mean_moment, mean_weight, pltpu.with_memory_space_constraint(moment, pltpu.HBM))
    return averaged.T, blended.T[None]


def solution(mesh):
    return jax.shard_map(
        body,
        mesh=mesh,
        in_specs=(
            P("rep", None, "shard"),
            P("rep", None, "shard"),
            P("rep", None, "shard", None),
            P("rep", None, None, "shard"),
            P("shard"),
        ),
        out_specs=(P(None, "shard"), P("rep", None, "shard")),
        check_vma=False,
    )
```

```python
import math

import jax
import jax.numpy as jnp
from jax import lax
from jax.experimental import pallas as pl
from jax.experimental.pallas import tpu as pltpu
from jax.sharding import PartitionSpec as P


D = 1600
TOP = D // 2
LANES = 128
SCALE = 1.0 / math.sqrt(D)
LEARN = 0.05
DECAY = 0.9


def rotated(up, cores):
    return [(2 * z + c, 2 * ((z + up) % 4) + (c + cores) % 2) for z in range(4) for c in range(2)]


def slope(pre, wanted):
    k = math.sqrt(2.0 / math.pi)
    square = pre * pre
    th = jnp.tanh(k * (pre + 0.044715 * pre * square))
    half = 0.5 * (1.0 + th)
    deriv = half + 0.5 * pre * (1.0 - th * th) * (k * (1.0 + 3 * 0.044715 * square))
    return (pre * half - wanted) * deriv * SCALE


def places(me, ups):
    z, c = me // 2, me % 2
    return [2 * ((z + up) % 4) + (c + k) % 2 for up in ups for k in range(2)]


UNITS = 80
LINES = 1024
FULL = D // LANES


def pack(lines, value):
    for j in range(FULL):
        lines[j * UNITS : (j + 1) * UNITS, :] = value[:, j * LANES : (j + 1) * LANES].astype(jnp.bfloat16)
    rest = value[:, FULL * LANES :]
    folded = jnp.concatenate([rest[: UNITS // 2], rest[UNITS // 2 :]], axis=1)
    at = FULL * UNITS
    lines[at : at + UNITS // 2, :] = folded.astype(jnp.bfloat16)
    at += UNITS // 2
    lines[at:, :] = jnp.zeros((LINES - at, LANES), jnp.bfloat16)


def unpacked(lines, at):
    for j in range(FULL):
        yield slice(j * LANES, (j + 1) * LANES), lines[pl.ds(at + j * UNITS, UNITS), :].astype(jnp.float32)
    rest = lines[pl.ds(at + FULL * UNITS, UNITS // 2), :].astype(jnp.float32)
    half = LANES // 2
    yield slice(FULL * LANES, D), jnp.concatenate([rest[:, :half], rest[:, half:]], axis=0)


def step_kernel(step, ups, late):
    first = step == 0

    def kernel(me, wanted, *refs):
        extra = 4 if first and late else 1
        refs, (x, g, m_buf, want, fetched, loaded, stored, *bufs) = refs[: -7 - extra], refs[-7 - extra :]
        if first and late:
            full, half, moment, *refs = refs
        elif first:
            full, moment, *refs = refs
        else:
            half, moment, *refs = refs
        count = 2 * len(ups) * (1 if step and not late else 2)
        blocks, outs = refs[:count], refs[count:]
        units = wanted.shape[1]
        lines, w_buf, w_half, m_half = bufs if len(bufs) == 4 else (bufs[0], bufs[0], None, None)
        loads = []
        if first:
            loads.append(pltpu.make_async_copy(full, w_buf, loaded.at[0]))
        if not (first and late):
            loads.append(pltpu.make_async_copy(moment, m_buf, loaded.at[1]))
        fetches = []
        for i, a in enumerate(places(me[0], ups)):
            lanes = slice(i * LANES, (i + 1) * LANES)
            theirs = wanted.at[step, :, pl.ds(pl.multiple_of(a * LANES, LANES), LANES)]
            moves = [(theirs, want.at[:, lanes])]
            if count == 2 * len(ups):
                moves.append((blocks[i], x.at[:, lanes]))
            else:
                moves += [(blocks[2 * i], x.at[:TOP, lanes]), (blocks[2 * i + 1], x.at[TOP:, lanes])]
            for k, (part, whole) in enumerate(moves):
                fetches.append(pltpu.make_async_copy(part, whole, fetched.at[i, k]))
        if first and not late:
            loads[0].start()
        for fetch in fetches:
            fetch.start()
        for load in loads[first and not late :]:
            load.start()
        for fetch in fetches:
            fetch.wait()
        if first and not late:
            loads[0].wait()
            half = outs[1]
            half[...] = w_buf[...].astype(jnp.bfloat16)
        pre = jnp.dot(half[...], x[...], preferred_element_type=jnp.float32) * SCALE
        hidden = slope(pre, want[...].astype(jnp.float32)).astype(jnp.bfloat16)
        g[...] = lax.dot_general(hidden, x[...], (((1,), (1,)), ((), ())), preferred_element_type=jnp.float32)
        for load in loads[first and not late :]:
            load.wait()
        copies = []
        for i in range(units // UNITS):
            rows, span = slice(i * UNITS, (i + 1) * UNITS), slice(i * LINES, (i + 1) * LINES)
            if first and late:
                m = moment[rows, :] + g[rows, :]
                w = w_buf[rows, :] - LEARN * m
                w_half[rows, :] = w.astype(jnp.bfloat16)
                m_half[rows, :] = m.astype(jnp.bfloat16)
                pack(lines.at[span, :], w)
                moves = [(lines, span), (w_half, rows), (m_half, rows)]
            elif first:
                outs[0][rows, :] = DECAY * m_buf[rows, :] + g[rows, :]
                moves = []
            elif late:
                pack(lines.at[span, :], m_buf[rows, :] + g[rows, :])
                moves = [(lines, span)]
            else:
                g[rows, :] = DECAY * m_buf[rows, :].astype(jnp.float32) + g[rows, :]
                moves = [(g, rows)]
            for o, (buf, part) in enumerate(moves):
                copy = pltpu.make_async_copy(buf.at[part, :], outs[o].at[part, :], stored.at[o, i])
                copy.start()
                copies.append(copy)
        for copy in copies:
            copy.wait()

    return kernel


def last_kernel(blend, lines, mean_weight, moment, averaged, blended, m_buf, w_buf, a_buf, b_buf, loaded, stored):
    loads, copies = [], []
    count = averaged.shape[0] // UNITS
    parts = [(slice(i * UNITS, (i + 1) * UNITS), slice(i * LINES, (i + 1) * LINES)) for i in range(count)]
    for i, (rows, span) in enumerate(parts):
        loads.append(
            [
                pltpu.make_async_copy(mean_weight.at[rows, :], w_buf.at[rows, :], loaded.at[0, i]),
                pltpu.make_async_copy(moment.at[span, :], m_buf.at[span, :], loaded.at[1, i]),
            ]
        )
        for load in loads[-1]:
            load.start()
    for i, (rows, span) in enumerate(parts):
        for load in loads[i]:
            load.wait()
        b = blend[rows, :]
        for (lanes, m), (_, own) in zip(unpacked(lines, i * LINES), unpacked(m_buf, i * LINES)):
            a_buf[rows, lanes] = w_buf[rows, lanes].astype(jnp.float32) - LEARN * m
            b_buf[rows, lanes] = b * m + (1.0 - b) * own
        for k, (buf, out) in enumerate([(a_buf, averaged), (b_buf, blended)]):
            copy = pltpu.make_async_copy(buf.at[rows, :], out.at[rows, :], stored.at[k, i])
            copy.start()
            copies.append(copy)
    for copy in copies:
        copy.wait()


ROUND = (0, 3, 1, 2)


def spread_kernel(me, *refs):
    *parts, out, lines = refs
    x, y, core = me[0] // 8, me[0] % 4, me[1] % 2
    rows = lines.shape[0] // 16
    for part, far in zip(parts, ROUND):
        for i, near in enumerate(ROUND):
            dx, dy = near + core * (far - near), far + core * (near - far)
            owner = (x + dy) % 4 * 4 + (y + dx) % 4
            lines[pl.ds(pl.multiple_of(owner * rows, rows), rows), :] = part[i * rows : (i + 1) * rows, :]
    for u in range(out.shape[0] // UNITS):
        for lanes, v in unpacked(lines, u * LINES):
            out[u * UNITS : (u + 1) * UNITS, lanes] = v.astype(jnp.bfloat16)


SMEM = pl.BlockSpec(memory_space=pltpu.SMEM)
VMEM = pl.BlockSpec(memory_space=pltpu.VMEM)
MIB = 1 << 20


FAR = pl.BlockSpec(memory_space=pltpu.HBM)


def kept(v):
    return pltpu.with_memory_space_constraint(v, pltpu.HBM)


def local_step(me, wanted, weights, moment, blocks, step, ups):
    first, late = step == 0, ups == (2,)
    units, tokens = wanted.shape[1], 2 * LANES * len(ups)
    whole, half = ((units, D), jnp.float32), ((units, D), jnp.bfloat16)
    lines = (units // UNITS * LINES, LANES), jnp.bfloat16
    outs = [[[whole], [lines]], [[whole, half], [lines, half, half]]][first][late]
    bufs = [lines if late else whole if first else ((8, LANES), jnp.bfloat16)]
    if first and late:
        bufs = [lines, whole, half, half]
    here = first and not late
    args = [kept(w) if w.dtype == jnp.float32 else w for w in weights]
    specs = [FAR if w.dtype == jnp.float32 else VMEM for w in weights]
    args.append(moment if first and late else kept(moment))
    specs.append(VMEM if first and late else FAR)
    return pl.pallas_call(
        step_kernel(step, ups, late),
        out_shape=tuple(jax.ShapeDtypeStruct(*o) if here else pltpu.HBM(*o) for o in outs),
        in_specs=[SMEM, FAR, *specs] + [pl.BlockSpec(memory_space=pl.ANY)] * len(blocks),
        out_specs=(VMEM if here else FAR,) * len(outs),
        scratch_shapes=[
            pltpu.VMEM((D, tokens), jnp.bfloat16),
            pltpu.VMEM(*whole),
            pltpu.VMEM(moment.shape, moment.dtype),
            pltpu.VMEM((units, tokens), jnp.bfloat16),
            pltpu.SemaphoreType.DMA((2 * len(ups), 3)),
            pltpu.SemaphoreType.DMA((2,)),
            pltpu.SemaphoreType.DMA((len(outs), units // UNITS)),
            *[pltpu.VMEM(*b) for b in bufs],
        ],
        cost_estimate=pl.CostEstimate(
            flops=4 * tokens * units * D, bytes_accessed=8 * units * D, transcendentals=tokens * units
        ),
        compiler_params=pltpu.CompilerParams(vmem_limit_bytes=24 * MIB),
    )(me, kept(wanted), *args, *blocks)


def gate_kernel(me, out):
    out[0] = me[0]


def gate(me):
    return pl.pallas_call(
        gate_kernel,
        out_shape=jax.ShapeDtypeStruct((1,), jnp.int32),
        in_specs=[SMEM],
        out_specs=SMEM,
        compiler_params=pltpu.CompilerParams(vmem_limit_bytes=MIB),
    )(me)


def shard_permute(v, up, cores):
    return lax.ppermute(v, "shard", rotated(up, cores))


def gather(piece):
    top, bottom = piece[:TOP], piece[TOP:]
    low_top = shard_permute(top, 1, 0)
    high_bottom = shard_permute(bottom, -1, 0)
    low_bottom = shard_permute(bottom, 1, 0)
    high_top = shard_permute(top, -1, 0)
    far = [shard_permute(low_top, 1, 0), shard_permute(high_bottom, -1, 0)]
    return both_cores([top, bottom, low_top, low_bottom, high_top, high_bottom]), both_cores(far), (low_bottom, high_top)


def gather_whole(piece):
    low, high = shard_permute(piece, 1, 0), shard_permute(piece, -1, 0)
    far = [shard_permute(low[:TOP], 1, 0), shard_permute(high[TOP:], -1, 0)]
    near = []
    for v in (piece, low, high):
        near += [v, shard_permute(v, 0, 1)]
    return near, both_cores(far)


def both_cores(values):
    swapped = [shard_permute(v, 0, 1) for v in values]
    out = []
    for i in range(0, len(values), 2):
        out += values[i : i + 2] + swapped[i : i + 2]
    return out


def added(got):
    return jnp.sum(got[...].astype(jnp.float32), axis=0)


def sum_kernel(got, out):
    out[...] = added(got).astype(jnp.bfloat16)


def mean_kernel(got, out):
    mean = (added(got) / got.shape[0]).astype(jnp.bfloat16)
    out[...] = jnp.broadcast_to(mean[None], out.shape)


def pair_kernel(here, there, out):
    out[...] = ((here[...].astype(jnp.float32) + there[...].astype(jnp.float32)) / 32).astype(jnp.bfloat16)


def small(kernel, args, shape):
    return pl.pallas_call(
        kernel,
        out_shape=jax.ShapeDtypeStruct(shape, jnp.bfloat16),
        in_specs=[VMEM] * len(args),
        out_specs=VMEM,
        compiler_params=pltpu.CompilerParams(vmem_limit_bytes=8 * MIB),
    )(*args)


def join_kernel(*refs):
    *parts, out = refs
    at = 0
    for part in parts:
        out[at : at + part.shape[0], :] = part[...]
        at += part.shape[0]


def replica_permute(v, core0, core1):
    pairs = []
    for r in range(32):
        for k in range(8):
            x, z, y = (core0, core1)[k % 2]
            to = 8 * ((r // 8 + x) % 4) + 4 * ((r // 4 + z) % 2) + (r + y) % 4
            pairs.append((8 * r + k, 8 * to + k))
    return lax.ppermute(v, ("rep", "shard"), pairs)


def weight_mean(lines):
    planes = [[8 * x + 4 * z + y for x in range(4) for y in range(4)] for z in range(2)]
    got = lax.all_to_all(lines.reshape(16, -1, LANES), "rep", 0, 0, axis_index_groups=planes)
    part = got.shape[1:]
    here = small(sum_kernel, [got], part)
    there = replica_permute(here, (0, 1, 0), (0, 1, 0))
    chunk = small(pair_kernel, [here, there], part)
    line = [replica_permute(chunk, (0, 0, k), (k, 0, 0)) for k in (1, 3, 2)]
    plane = small(join_kernel, [chunk, *line], (4 * part[0], LANES))
    return [plane] + [replica_permute(plane, (k, 0, 0), (0, 0, k)) for k in (1, 3, 2)]


def body(params, momentum, tokens, targets, blend_weight):
    weight = params[0].T
    moment = momentum[0].T
    units = weight.shape[0]
    pieces = jnp.swapaxes(tokens[0], 1, 2)
    wanted = jnp.swapaxes(targets[0], 1, 2)
    me = lax.axis_index("shard")[None]
    replicas = lax.axis_size("rep")
    rows = units // UNITS * LINES

    whole = jax.ShapeDtypeStruct((units, D), jnp.float32)
    half = jax.ShapeDtypeStruct((units, D), jnp.bfloat16)

    near, far, sent = gather(pieces[0])
    second, _ = lax.optimization_barrier((pieces[1], sent))
    near2, far2 = gather_whole(second)

    ready = gate(me)
    moment, old = local_step(ready, wanted, [weight], moment, near, 0, (0, 3, 1))
    weight_lines, weight, moment = local_step(me, wanted, [weight, old], moment, far, 0, (2,))
    parts = weight_mean(weight_lines)

    (moment,) = local_step(me, wanted, [weight], moment, near2, 1, (0, 3, 1))
    (moment_lines,) = local_step(me, wanted, [weight], moment, far2, 1, (2,))
    got = lax.all_to_all(moment_lines.reshape(replicas, -1, LANES), "rep", 0, 0)
    means = small(mean_kernel, [got], got.shape)
    mean_moment = lax.all_to_all(means, "rep", 0, 0).reshape(-1, LANES)

    mean_weight = pl.pallas_call(
        spread_kernel,
        out_shape=pltpu.HBM(half.shape, half.dtype),
        in_specs=[SMEM] + [VMEM] * 4,
        out_specs=VMEM,
        scratch_shapes=[pltpu.VMEM((rows, LANES), jnp.bfloat16)],
        compiler_params=pltpu.CompilerParams(vmem_limit_bytes=12 * MIB),
        name="spread",
    )(jnp.stack([lax.axis_index("rep"), lax.axis_index("shard")]), *parts)
    averaged, blended = pl.pallas_call(
        last_kernel,
        out_shape=(whole, whole),
        in_specs=[VMEM, VMEM, FAR, FAR],
        out_specs=(FAR, FAR),
        scratch_shapes=[
            pltpu.VMEM((rows, LANES), jnp.bfloat16),
            pltpu.VMEM((units, D), jnp.bfloat16),
            pltpu.VMEM((units, D), jnp.float32),
            pltpu.VMEM((units, D), jnp.float32),
            pltpu.SemaphoreType.DMA((2, units // UNITS)),
            pltpu.SemaphoreType.DMA((2, units // UNITS)),
        ],
        compiler_params=pltpu.CompilerParams(vmem_limit_bytes=16 * MIB),
        name="last",
    )(blend_weight[:, None], mean_moment, kept(mean_weight), kept(moment_lines))
    return averaged.T, blended.T[None]


def solution(mesh):
    return jax.shard_map(
        body,
        mesh=mesh,
        in_specs=(
            P("rep", None, "shard"),
            P("rep", None, "shard"),
            P("rep", None, "shard", None),
            P("rep", None, None, "shard"),
            P("shard"),
        ),
        out_specs=(P(None, "shard"), P("rep", None, "shard")),
        check_vma=False,
    )
```

```python
import math

import jax
import jax.numpy as jnp
from jax import lax
from jax.experimental import pallas as pl
from jax.experimental.pallas import tpu as pltpu
from jax.sharding import PartitionSpec as P


D = 1600
TOP = D // 2
LANES = 128
SCALE = 1.0 / math.sqrt(D)
LEARN = 0.05
DECAY = 0.9


def rotated(up, cores):
    return [(2 * z + c, 2 * ((z + up) % 4) + (c + cores) % 2) for z in range(4) for c in range(2)]


def slope(pre, wanted):
    k = math.sqrt(2.0 / math.pi)
    square = pre * pre
    th = jnp.tanh(k * (pre + 0.044715 * pre * square))
    half = 0.5 * (1.0 + th)
    deriv = half + 0.5 * pre * (1.0 - th * th) * (k * (1.0 + 3 * 0.044715 * square))
    return (pre * half - wanted) * deriv * SCALE


def places(me, ups, apart):
    z, c = me // 2, me % 2
    return [2 * ((z + (up * (2 * q - 1) if apart else up) + 8) % 4) + q for up in ups for q in (c, 1 - c)]


UNITS = 80
LINES = 1024
FULL = D // LANES


def pack(lines, value):
    for j in range(FULL):
        lines[j * UNITS : (j + 1) * UNITS, :] = value[:, j * LANES : (j + 1) * LANES].astype(jnp.bfloat16)
    rest = value[:, FULL * LANES :]
    folded = jnp.concatenate([rest[: UNITS // 2], rest[UNITS // 2 :]], axis=1)
    at = FULL * UNITS
    lines[at : at + UNITS // 2, :] = folded.astype(jnp.bfloat16)
    at += UNITS // 2
    lines[at:, :] = jnp.zeros((LINES - at, LANES), jnp.bfloat16)


def unpacked(lines, at):
    for j in range(FULL):
        yield slice(j * LANES, (j + 1) * LANES), lines[pl.ds(at + j * UNITS, UNITS), :].astype(jnp.float32)
    rest = lines[pl.ds(at + FULL * UNITS, UNITS // 2), :].astype(jnp.float32)
    half = LANES // 2
    yield slice(FULL * LANES, D), jnp.concatenate([rest[:, :half], rest[:, half:]], axis=0)


def step_kernel(step, ups, late):
    first = step == 0

    def kernel(me, wanted, *refs):
        extra = 4 if first and late else 1
        refs, (x, g, m_buf, want, fetched, loaded, stored, *bufs) = refs[: -7 - extra], refs[-7 - extra :]
        full = half = None
        if first:
            full, *refs = refs
        if late or not first:
            half, *refs = refs
        moment, *refs = refs
        count = 2 * len(ups) * (2 - step)
        blocks, outs = refs[:count], refs[count:]
        units = wanted.shape[1]
        fetches = []
        for i, a in enumerate(places(me[0], ups, step == 1)):
            lanes = slice(i * LANES, (i + 1) * LANES)
            moves = [(wanted.at[step, :, pl.ds(pl.multiple_of(a * LANES, LANES), LANES)], want.at[:, lanes])]
            if count == 2 * len(ups):
                moves.append((blocks[i], x.at[:, lanes]))
            else:
                moves += [(blocks[2 * i], x.at[:TOP, lanes]), (blocks[2 * i + 1], x.at[TOP:, lanes])]
            fetches.append([pltpu.make_async_copy(*m, fetched.at[i, k]) for k, m in enumerate(moves)])
        loads = []
        if first:
            w_buf = bufs[1 if late else 0]
            loads.append(pltpu.make_async_copy(full, w_buf, loaded.at[0]))
        if not late:
            loads.append(pltpu.make_async_copy(moment, m_buf, loaded.at[1]))
        if first and not late:
            loads[0].start()
        for fetch in fetches:
            for copy in fetch:
                copy.start()
        for load in loads[first and not late :]:
            load.start()
        if first and not late:
            loads.pop(0).wait()
            half = outs[1]
            half[...] = w_buf[...].astype(jnp.bfloat16)
        for fetch in fetches:
            for copy in fetch:
                copy.wait()
        pre = jnp.dot(half[...], x[...], preferred_element_type=jnp.float32) * SCALE
        hidden = slope(pre, want[...].astype(jnp.float32)).astype(jnp.bfloat16)
        for load in loads:
            load.wait()
        grad = lax.dot_general(hidden, x[...], (((1,), (1,)), ((), ())), preferred_element_type=jnp.float32)
        if not late:
            outs[0][...] = DECAY * m_buf[...].astype(jnp.float32) + grad
            return
        g[...] = grad
        lines = bufs[0]
        copies = []
        for i in range(units // UNITS):
            rows, span = slice(i * UNITS, (i + 1) * UNITS), slice(i * LINES, (i + 1) * LINES)
            m = moment[rows, :] + g[rows, :]
            moves = [(lines, span)]
            if first:
                _, w_buf, w_half, m_half = bufs
                w_half[rows, :] = (w_buf[rows, :] - LEARN * m).astype(jnp.bfloat16)
                m_half[rows, :] = m.astype(jnp.bfloat16)
                moves += [(w_half, rows), (m_half, rows)]
                m = w_half[rows, :]
            pack(lines.at[span, :], m)
            for o, (buf, part) in enumerate(moves):
                copy = pltpu.make_async_copy(buf.at[part, :], outs[o].at[part, :], stored.at[o, i])
                copy.start()
                copies.append(copy)
        for copy in copies:
            copy.wait()

    return kernel


def put_out(buf, out, rows, sem):
    copy = pltpu.make_async_copy(buf.at[rows, :], out.at[rows, :], sem)
    copy.start()
    return copy


def blend_kernel(blend, lines, moment, blended, m_buf, b_buf, loaded, stored):
    count = blended.shape[0] // UNITS
    spans = [slice(i * LINES, (i + 1) * LINES) for i in range(count)]
    loads = [pltpu.make_async_copy(moment.at[p, :], m_buf.at[p, :], loaded.at[i]) for i, p in enumerate(spans)]
    for load in loads:
        load.start()
    copies = []
    for i in range(count):
        loads[i].wait()
        rows = slice(i * UNITS, (i + 1) * UNITS)
        b = blend[rows, :]
        for (lanes, m), (_, own) in zip(unpacked(lines, i * LINES), unpacked(m_buf, i * LINES)):
            b_buf[rows, lanes] = b * m + (1.0 - b) * own
        copies.append(put_out(b_buf, blended, rows, stored.at[i]))
    for copy in copies:
        copy.wait()


ROUND = (0, 3, 1, 2)


def average_kernel(rep, me, lines, *refs):
    *parts, averaged, w_lines, a_buf, stored = refs
    x, y, core = rep[0] // 8, rep[0] % 4, me[0] % 2
    chunk = lines.shape[0] // 16
    for part, far in zip(parts, ROUND):
        for i, near in enumerate(ROUND):
            dx, dy = near + core * (far - near), far + core * (near - far)
            owner = (x + dy) % 4 * 4 + (y + dx) % 4
            w_lines[pl.ds(pl.multiple_of(owner * chunk, chunk), chunk), :] = part[i * chunk : (i + 1) * chunk, :]
    copies = []
    for i in range(averaged.shape[0] // UNITS):
        rows = slice(i * UNITS, (i + 1) * UNITS)
        for (lanes, w), (_, m) in zip(unpacked(w_lines, i * LINES), unpacked(lines, i * LINES)):
            a_buf[rows, lanes] = w - LEARN * m
        copies.append(put_out(a_buf, averaged, rows, stored.at[i]))
    for copy in copies:
        copy.wait()


SMEM = pl.BlockSpec(memory_space=pltpu.SMEM)
VMEM = pl.BlockSpec(memory_space=pltpu.VMEM)
MIB = 1 << 20


FAR = pl.BlockSpec(memory_space=pltpu.HBM)


def kept(v):
    return pltpu.with_memory_space_constraint(v, pltpu.HBM)


def local_step(me, wanted, weights, moment, blocks, step, ups):
    first, late = step == 0, ups == (2,)
    units, tokens = wanted.shape[1], 2 * LANES * len(ups)
    whole, half = ((units, D), jnp.float32), ((units, D), jnp.bfloat16)
    lines = (units // UNITS * LINES, LANES), jnp.bfloat16
    outs = [[[whole], [lines]], [[whole, half], [lines, half, half]]][first][late]
    small = (8, LANES), jnp.float32
    bufs = [lines if late else whole if first else small]
    if first and late:
        bufs = [lines, whole, half, half]
    args = [kept(w) if w.dtype == jnp.float32 else w for w in weights]
    specs = [FAR if w.dtype == jnp.float32 else VMEM for w in weights]
    args.append(moment if late else kept(moment))
    specs.append(VMEM if late else FAR)
    return pl.pallas_call(
        step_kernel(step, ups, late),
        out_shape=tuple((pltpu.HBM if late else jax.ShapeDtypeStruct)(*o) for o in outs),
        in_specs=[SMEM, FAR, *specs] + [pl.BlockSpec(memory_space=pl.ANY)] * len(blocks),
        out_specs=(FAR if late else VMEM,) * len(outs),
        scratch_shapes=[
            pltpu.VMEM((D, tokens), jnp.bfloat16),
            pltpu.VMEM(*(whole if late else small)),
            pltpu.VMEM(*(small if late else (moment.shape, moment.dtype))),
            pltpu.VMEM((units, tokens), jnp.bfloat16),
            pltpu.SemaphoreType.DMA((2 * len(ups), 3)),
            pltpu.SemaphoreType.DMA((2,)),
            pltpu.SemaphoreType.DMA((len(outs), units // UNITS)),
            *[pltpu.VMEM(*b) for b in bufs],
        ],
        cost_estimate=pl.CostEstimate(
            flops=4 * tokens * units * D, bytes_accessed=8 * units * D, transcendentals=tokens * units
        ),
        compiler_params=pltpu.CompilerParams(vmem_limit_bytes=24 * MIB),
    )(me, kept(wanted), *args, *blocks)


def gate_kernel(me, out):
    out[0] = me[0]


def gate(me):
    return pl.pallas_call(
        gate_kernel,
        out_shape=jax.ShapeDtypeStruct((1,), jnp.int32),
        in_specs=[SMEM],
        out_specs=SMEM,
        compiler_params=pltpu.CompilerParams(vmem_limit_bytes=MIB),
    )(me)


def shard_permute(v, up, cores):
    return lax.ppermute(v, "shard", rotated(up, cores))


def gather(piece):
    top, bottom = piece[:TOP], piece[TOP:]
    low_top = shard_permute(top, 1, 0)
    high_bottom = shard_permute(bottom, -1, 0)
    low_bottom = shard_permute(bottom, 1, 0)
    high_top = shard_permute(top, -1, 0)
    far = [shard_permute(low_top, 1, 0), shard_permute(high_bottom, -1, 0)]
    return both_cores([top, bottom, low_top, low_bottom, high_top, high_bottom]), both_cores(far), (low_bottom, high_top)


def gather_whole(piece):
    def passed(v, up):
        pairs = [(2 * z + c, 2 * ((z + up * (1 - 2 * c)) % 4) + c) for z in range(4) for c in range(2)]
        return lax.ppermute(v, "shard", pairs)

    one = passed(piece, 1)
    back = passed(piece, -1)
    two = passed(one, 1)
    near = []
    for v in (piece, one, back):
        near += [v, shard_permute(v, 0, 1)]
    return near, [two, shard_permute(two, 0, 1)]


def both_cores(values):
    swapped = [shard_permute(v, 0, 1) for v in values]
    out = []
    for i in range(0, len(values), 2):
        out += values[i : i + 2] + swapped[i : i + 2]
    return out


def added(got):
    return jnp.sum(got[...].astype(jnp.float32), axis=0)


def sum_kernel(got, out):
    out[...] = added(got).astype(jnp.bfloat16)


def mean_kernel(got, out):
    mean = (added(got) / got.shape[0]).astype(jnp.bfloat16)
    out[...] = jnp.broadcast_to(mean[None], out.shape)


def pair_kernel(here, there, out):
    out[...] = ((here[...].astype(jnp.float32) + there[...].astype(jnp.float32)) / 32).astype(jnp.bfloat16)


def small(kernel, args, shape):
    return pl.pallas_call(
        kernel,
        out_shape=jax.ShapeDtypeStruct(shape, jnp.bfloat16),
        in_specs=[VMEM] * len(args),
        out_specs=VMEM,
        compiler_params=pltpu.CompilerParams(vmem_limit_bytes=8 * MIB),
    )(*args)


def join_kernel(*refs):
    *parts, out = refs
    at = 0
    for part in parts:
        out[at : at + part.shape[0], :] = part[...]
        at += part.shape[0]


def replica_permute(v, core0, core1):
    pairs = []
    for r in range(32):
        for k in range(8):
            x, z, y = (core0, core1)[k % 2]
            to = 8 * ((r // 8 + x) % 4) + 4 * ((r // 4 + z) % 2) + (r + y) % 4
            pairs.append((8 * r + k, 8 * to + k))
    return lax.ppermute(v, ("rep", "shard"), pairs)


def weight_mean(lines):
    planes = [[8 * x + 4 * z + y for x in range(4) for y in range(4)] for z in range(2)]
    got = lax.all_to_all(lines.reshape(16, -1, LANES), "rep", 0, 0, axis_index_groups=planes)
    part = got.shape[1:]
    here = small(sum_kernel, [got], part)
    there = replica_permute(here, (0, 1, 0), (0, 1, 0))
    chunk = small(pair_kernel, [here, there], part)
    line = [replica_permute(chunk, (0, 0, k), (k, 0, 0)) for k in (1, 3, 2)]
    plane = small(join_kernel, [chunk, *line], (4 * part[0], LANES))
    return [plane] + [replica_permute(plane, (k, 0, 0), (0, 0, k)) for k in (1, 3, 2)]


def body(params, momentum, tokens, targets, blend_weight):
    weight = params[0].T
    moment = momentum[0].T
    units = weight.shape[0]
    pieces = jnp.swapaxes(tokens[0], 1, 2)
    wanted = jnp.swapaxes(targets[0], 1, 2)
    me = lax.axis_index("shard")[None]
    replicas = lax.axis_size("rep")
    rows = units // UNITS * LINES

    whole = jax.ShapeDtypeStruct((units, D), jnp.float32)

    near, far, sent = gather(pieces[0])
    second = pieces[1]
    second, _ = lax.optimization_barrier((second, sent))
    near2, far2 = gather_whole(second)

    ready = gate(me)
    moment, old = local_step(ready, wanted, [weight], moment, near, 0, (0, 3, 1))
    weight_lines, weight, moment = local_step(me, wanted, [weight, old], moment, far, 0, (2,))
    parts = weight_mean(weight_lines)

    (moment,) = local_step(me, wanted, [weight], moment, near2, 1, (0, 1, -1))
    (moment_lines,) = local_step(me, wanted, [weight], moment, far2, 1, (2,))
    got = lax.all_to_all(moment_lines.reshape(replicas, -1, LANES), "rep", 0, 0)
    means = small(mean_kernel, [got], got.shape)
    mean_moment = lax.all_to_all(means, "rep", 0, 0).reshape(-1, LANES)

    blended = pl.pallas_call(
        blend_kernel,
        out_shape=whole,
        in_specs=[VMEM, VMEM, FAR],
        out_specs=FAR,
        scratch_shapes=[
            pltpu.VMEM((rows, LANES), jnp.bfloat16),
            pltpu.VMEM((units, D), jnp.float32),
            pltpu.SemaphoreType.DMA((units // UNITS,)),
            pltpu.SemaphoreType.DMA((units // UNITS,)),
        ],
        compiler_params=pltpu.CompilerParams(vmem_limit_bytes=12 * MIB),
        name="blended",
    )(blend_weight[:, None], mean_moment, kept(moment_lines))
    averaged = pl.pallas_call(
        average_kernel,
        out_shape=whole,
        in_specs=[SMEM, SMEM] + [VMEM] * 5,
        out_specs=FAR,
        scratch_shapes=[
            pltpu.VMEM((rows, LANES), jnp.bfloat16),
            pltpu.VMEM((units, D), jnp.float32),
            pltpu.SemaphoreType.DMA((units // UNITS,)),
        ],
        compiler_params=pltpu.CompilerParams(vmem_limit_bytes=12 * MIB),
        name="averaged",
    )(gate(lax.axis_index("rep")[None]), me, mean_moment, *parts)
    return averaged.T, blended.T[None]


def solution(mesh):
    return jax.shard_map(
        body,
        mesh=mesh,
        in_specs=(
            P("rep", None, "shard"),
            P("rep", None, "shard"),
            P("rep", None, "shard", None),
            P("rep", None, None, "shard"),
            P("shard"),
        ),
        out_specs=(P(None, "shard"), P("rep", None, "shard")),
        check_vma=False,
    )
```

```python
import math

import jax
import jax.numpy as jnp
from jax import lax
from jax.experimental import pallas as pl
from jax.experimental.pallas import tpu as pltpu
from jax.sharding import PartitionSpec as P


D = 1600
TOP = D // 2
LANES = 128
SCALE = 1.0 / math.sqrt(D)
LEARN = 0.05
DECAY = 0.9


def rotated(up, cores):
    return [(2 * z + c, 2 * ((z + up) % 4) + (c + cores) % 2) for z in range(4) for c in range(2)]


def slope(pre, wanted):
    k = math.sqrt(2.0 / math.pi)
    square = pre * pre
    th = jnp.tanh(k * (pre + 0.044715 * pre * square))
    half = 0.5 * (1.0 + th)
    deriv = half + 0.5 * pre * (1.0 - th * th) * (k * (1.0 + 3 * 0.044715 * square))
    return (pre * half - wanted) * deriv * SCALE


def places(me, ups, apart):
    z, c = me // 2, me % 2
    return [2 * ((z + (up * (2 * q - 1) if apart else up) + 8) % 4) + q for up in ups for q in (c, 1 - c)]


UNITS = 80
LINES = 1024
FULL = D // LANES


def pack(lines, value):
    for j in range(FULL):
        lines[j * UNITS : (j + 1) * UNITS, :] = value[:, j * LANES : (j + 1) * LANES].astype(jnp.bfloat16)
    rest = value[:, FULL * LANES :]
    folded = jnp.concatenate([rest[: UNITS // 2], rest[UNITS // 2 :]], axis=1)
    at = FULL * UNITS
    lines[at : at + UNITS // 2, :] = folded.astype(jnp.bfloat16)
    at += UNITS // 2
    lines[at:, :] = jnp.zeros((LINES - at, LANES), jnp.bfloat16)


def unpacked(lines, at):
    for j in range(FULL):
        yield slice(j * LANES, (j + 1) * LANES), lines[pl.ds(at + j * UNITS, UNITS), :].astype(jnp.float32)
    rest = lines[pl.ds(at + FULL * UNITS, UNITS // 2), :].astype(jnp.float32)
    half = LANES // 2
    yield slice(FULL * LANES, D), jnp.concatenate([rest[:, :half], rest[:, half:]], axis=0)


def step_kernel(step, ups, late):
    first = step == 0

    def kernel(me, wanted, *refs):
        extra = 4 if first and late else 1
        refs, (x, g, m_buf, want, fetched, loaded, stored, *bufs) = refs[: -7 - extra], refs[-7 - extra :]
        if first and late:
            full, *refs = refs
        half, moment, *refs = refs
        count = 2 * len(ups) * (2 - step)
        blocks, outs = refs[:count], refs[count:]
        units = wanted.shape[1]
        fetches = []
        for i, a in enumerate(places(me[0], ups, step == 1)):
            lanes = slice(i * LANES, (i + 1) * LANES)
            moves = [(wanted.at[step, :, pl.ds(pl.multiple_of(a * LANES, LANES), LANES)], want.at[:, lanes])]
            if count == 2 * len(ups):
                moves.append((blocks[i], x.at[:, lanes]))
            else:
                moves += [(blocks[2 * i], x.at[:TOP, lanes]), (blocks[2 * i + 1], x.at[TOP:, lanes])]
            fetches.append([pltpu.make_async_copy(*m, fetched.at[i, k]) for k, m in enumerate(moves)])
        loads = []
        if first and late:
            w_buf = bufs[1]
            loads.append(pltpu.make_async_copy(full, w_buf, loaded.at[0]))
        if not late:
            loads.append(pltpu.make_async_copy(moment, m_buf, loaded.at[1]))
        for fetch in fetches:
            for copy in fetch:
                copy.start()
        for load in loads:
            load.start()
        for fetch in fetches:
            for copy in fetch:
                copy.wait()
        pre = jnp.dot(half[...], x[...], preferred_element_type=jnp.float32) * SCALE
        hidden = slope(pre, want[...].astype(jnp.float32)).astype(jnp.bfloat16)
        for load in loads:
            load.wait()
        grad = lax.dot_general(hidden, x[...], (((1,), (1,)), ((), ())), preferred_element_type=jnp.float32)
        if not late:
            outs[0][...] = DECAY * m_buf[...].astype(jnp.float32) + grad
            return
        g[...] = grad
        lines = bufs[0]
        copies = []
        for i in range(units // UNITS):
            rows, span = slice(i * UNITS, (i + 1) * UNITS), slice(i * LINES, (i + 1) * LINES)
            m = moment[rows, :] + g[rows, :]
            moves = [(lines, span)]
            if first:
                _, w_buf, w_half, m_half = bufs
                w_half[rows, :] = (w_buf[rows, :] - LEARN * m).astype(jnp.bfloat16)
                m_half[rows, :] = m.astype(jnp.bfloat16)
                moves += [(w_half, rows), (m_half, rows)]
                m = w_half[rows, :]
            pack(lines.at[span, :], m)
            for o, (buf, part) in enumerate(moves):
                copy = pltpu.make_async_copy(buf.at[part, :], outs[o].at[part, :], stored.at[o, i])
                copy.start()
                copies.append(copy)
        for copy in copies:
            copy.wait()

    return kernel


def put_out(buf, out, rows, sem):
    copy = pltpu.make_async_copy(buf.at[rows, :], out.at[rows, :], sem)
    copy.start()
    return copy


def blend_kernel(blend, lines, moment, blended, m_buf, b_buf, loaded, stored):
    count = blended.shape[0] // UNITS
    spans = [slice(i * LINES, (i + 1) * LINES) for i in range(count)]
    loads = [pltpu.make_async_copy(moment.at[p, :], m_buf.at[p, :], loaded.at[i]) for i, p in enumerate(spans)]
    for load in loads:
        load.start()
    copies = []
    for i in range(count):
        loads[i].wait()
        rows = slice(i * UNITS, (i + 1) * UNITS)
        b = blend[rows, :]
        for (lanes, m), (_, own) in zip(unpacked(lines, i * LINES), unpacked(m_buf, i * LINES)):
            b_buf[rows, lanes] = b * m + (1.0 - b) * own
        copies.append(put_out(b_buf, blended, rows, stored.at[i]))
    for copy in copies:
        copy.wait()


ROUND = (0, 3, 1, 2)


def average_kernel(rep, me, lines, *refs):
    *parts, averaged, w_lines, a_buf, stored = refs
    x, y, core = rep[0] // 8, rep[0] % 4, me[0] % 2
    chunk = lines.shape[0] // 16
    for part, far in zip(parts, ROUND):
        for i, near in enumerate(ROUND):
            dx, dy = near + core * (far - near), far + core * (near - far)
            owner = (x + dy) % 4 * 4 + (y + dx) % 4
            w_lines[pl.ds(pl.multiple_of(owner * chunk, chunk), chunk), :] = part[i * chunk : (i + 1) * chunk, :]
    copies = []
    for i in range(averaged.shape[0] // UNITS):
        rows = slice(i * UNITS, (i + 1) * UNITS)
        for (lanes, w), (_, m) in zip(unpacked(w_lines, i * LINES), unpacked(lines, i * LINES)):
            a_buf[rows, lanes] = w - LEARN * m
        copies.append(put_out(a_buf, averaged, rows, stored.at[i]))
    for copy in copies:
        copy.wait()


SMEM = pl.BlockSpec(memory_space=pltpu.SMEM)
VMEM = pl.BlockSpec(memory_space=pltpu.VMEM)
MIB = 1 << 20


FAR = pl.BlockSpec(memory_space=pltpu.HBM)


def kept(v):
    return pltpu.with_memory_space_constraint(v, pltpu.HBM)


def local_step(me, wanted, weights, moment, blocks, step, ups):
    first, late = step == 0, ups == (2,)
    units, tokens = wanted.shape[1], 2 * LANES * len(ups)
    whole, half = ((units, D), jnp.float32), ((units, D), jnp.bfloat16)
    lines = (units // UNITS * LINES, LANES), jnp.bfloat16
    outs = [whole] if not late else [lines, half, half] if first else [lines]
    small = (8, LANES), jnp.float32
    bufs = [lines if late else small]
    if first and late:
        bufs = [lines, whole, half, half]
    args = [kept(w) if w.dtype == jnp.float32 else w for w in weights]
    specs = [FAR if w.dtype == jnp.float32 else VMEM for w in weights]
    args.append(moment if late else kept(moment))
    specs.append(VMEM if late else FAR)
    return pl.pallas_call(
        step_kernel(step, ups, late),
        out_shape=tuple((pltpu.HBM if late else jax.ShapeDtypeStruct)(*o) for o in outs),
        in_specs=[SMEM, FAR, *specs] + [pl.BlockSpec(memory_space=pl.ANY)] * len(blocks),
        out_specs=(FAR if late else VMEM,) * len(outs),
        scratch_shapes=[
            pltpu.VMEM((D, tokens), jnp.bfloat16),
            pltpu.VMEM(*(whole if late else small)),
            pltpu.VMEM(*(small if late else (moment.shape, moment.dtype))),
            pltpu.VMEM((units, tokens), jnp.bfloat16),
            pltpu.SemaphoreType.DMA((2 * len(ups), 3)),
            pltpu.SemaphoreType.DMA((2,)),
            pltpu.SemaphoreType.DMA((len(outs), units // UNITS)),
            *[pltpu.VMEM(*b) for b in bufs],
        ],
        cost_estimate=pl.CostEstimate(
            flops=4 * tokens * units * D, bytes_accessed=8 * units * D, transcendentals=tokens * units
        ),
        compiler_params=pltpu.CompilerParams(vmem_limit_bytes=24 * MIB),
    )(me, kept(wanted), *args, *blocks)


def half_kernel(weight, out):
    out[...] = weight[...].astype(jnp.bfloat16)


def gate_kernel(me, out):
    out[0] = me[0]


def gate(me):
    return pl.pallas_call(
        gate_kernel,
        out_shape=jax.ShapeDtypeStruct((1,), jnp.int32),
        in_specs=[SMEM],
        out_specs=SMEM,
        compiler_params=pltpu.CompilerParams(vmem_limit_bytes=MIB),
    )(me)


def shard_permute(v, up, cores):
    return lax.ppermute(v, "shard", rotated(up, cores))


def gather(piece):
    top, bottom = piece[:TOP], piece[TOP:]
    low_top = shard_permute(top, 1, 0)
    high_bottom = shard_permute(bottom, -1, 0)
    low_bottom = shard_permute(bottom, 1, 0)
    high_top = shard_permute(top, -1, 0)
    far = [shard_permute(low_top, 1, 0), shard_permute(high_bottom, -1, 0)]
    return both_cores([top, bottom, low_top, low_bottom, high_top, high_bottom]), both_cores(far), (low_bottom, high_top)


def gather_whole(piece):
    def passed(v, up):
        pairs = [(2 * z + c, 2 * ((z + up * (1 - 2 * c)) % 4) + c) for z in range(4) for c in range(2)]
        return lax.ppermute(v, "shard", pairs)

    one = passed(piece, 1)
    back = passed(piece, -1)
    two = passed(one, 1)
    near = []
    for v in (piece, one, back):
        near += [v, shard_permute(v, 0, 1)]
    return near, [two, shard_permute(two, 0, 1)]


def both_cores(values):
    swapped = [shard_permute(v, 0, 1) for v in values]
    out = []
    for i in range(0, len(values), 2):
        out += values[i : i + 2] + swapped[i : i + 2]
    return out


def added(got):
    return jnp.sum(got[...].astype(jnp.float32), axis=0)


def sum_kernel(got, out):
    out[...] = added(got).astype(jnp.bfloat16)


def mean_kernel(got, out):
    mean = (added(got) / got.shape[0]).astype(jnp.bfloat16)
    out[...] = jnp.broadcast_to(mean[None], out.shape)


def pair_kernel(here, there, out):
    out[...] = ((here[...].astype(jnp.float32) + there[...].astype(jnp.float32)) / 32).astype(jnp.bfloat16)


def small(kernel, args, shape):
    return pl.pallas_call(
        kernel,
        out_shape=jax.ShapeDtypeStruct(shape, jnp.bfloat16),
        in_specs=[VMEM] * len(args),
        out_specs=VMEM,
        compiler_params=pltpu.CompilerParams(vmem_limit_bytes=8 * MIB),
    )(*args)


def join_kernel(*refs):
    *parts, out = refs
    at = 0
    for part in parts:
        out[at : at + part.shape[0], :] = part[...]
        at += part.shape[0]


def replica_permute(v, core0, core1):
    pairs = []
    for r in range(32):
        for k in range(8):
            x, z, y = (core0, core1)[k % 2]
            to = 8 * ((r // 8 + x) % 4) + 4 * ((r // 4 + z) % 2) + (r + y) % 4
            pairs.append((8 * r + k, 8 * to + k))
    return lax.ppermute(v, ("rep", "shard"), pairs)


def weight_mean(lines):
    planes = [[8 * x + 4 * z + y for x in range(4) for y in range(4)] for z in range(2)]
    got = lax.all_to_all(lines.reshape(16, -1, LANES), "rep", 0, 0, axis_index_groups=planes)
    part = got.shape[1:]
    here = small(sum_kernel, [got], part)
    there = replica_permute(here, (0, 1, 0), (0, 1, 0))
    chunk = small(pair_kernel, [here, there], part)
    line = [replica_permute(chunk, (0, 0, k), (k, 0, 0)) for k in (1, 3, 2)]
    plane = small(join_kernel, [chunk, *line], (4 * part[0], LANES))
    return [plane] + [replica_permute(plane, (k, 0, 0), (0, 0, k)) for k in (1, 3, 2)]


def body(params, momentum, tokens, targets, blend_weight):
    weight = params[0].T
    moment = momentum[0].T
    units = weight.shape[0]
    pieces = jnp.swapaxes(tokens[0], 1, 2)
    wanted = jnp.swapaxes(targets[0], 1, 2)
    me = lax.axis_index("shard")[None]
    replicas = lax.axis_size("rep")
    rows = units // UNITS * LINES

    whole = jax.ShapeDtypeStruct((units, D), jnp.float32)

    near, far, sent = gather(pieces[0])
    second = pieces[1]
    second, _ = lax.optimization_barrier((second, sent))
    near2, far2 = gather_whole(second)

    ready = gate(me)
    old = small(half_kernel, [weight], (units, D))
    (moment,) = local_step(ready, wanted, [old], moment, near, 0, (0, 3, 1))
    weight_lines, weight, moment = local_step(me, wanted, [weight, old], moment, far, 0, (2,))
    parts = weight_mean(weight_lines)

    (moment,) = local_step(me, wanted, [weight], moment, near2, 1, (0, 1, -1))
    (moment_lines,) = local_step(me, wanted, [weight], moment, far2, 1, (2,))
    got = lax.all_to_all(moment_lines.reshape(replicas, -1, LANES), "rep", 0, 0)
    means = small(mean_kernel, [got], got.shape)
    mean_moment = lax.all_to_all(means, "rep", 0, 0).reshape(-1, LANES)

    blended = pl.pallas_call(
        blend_kernel,
        out_shape=whole,
        in_specs=[VMEM, VMEM, FAR],
        out_specs=FAR,
        scratch_shapes=[
            pltpu.VMEM((rows, LANES), jnp.bfloat16),
            pltpu.VMEM((units, D), jnp.float32),
            pltpu.SemaphoreType.DMA((units // UNITS,)),
            pltpu.SemaphoreType.DMA((units // UNITS,)),
        ],
        compiler_params=pltpu.CompilerParams(vmem_limit_bytes=12 * MIB),
        name="blended",
    )(blend_weight[:, None], mean_moment, kept(moment_lines))
    averaged = pl.pallas_call(
        average_kernel,
        out_shape=whole,
        in_specs=[SMEM, SMEM] + [VMEM] * 5,
        out_specs=FAR,
        scratch_shapes=[
            pltpu.VMEM((rows, LANES), jnp.bfloat16),
            pltpu.VMEM((units, D), jnp.float32),
            pltpu.SemaphoreType.DMA((units // UNITS,)),
        ],
        compiler_params=pltpu.CompilerParams(vmem_limit_bytes=12 * MIB),
        name="averaged",
    )(gate(lax.axis_index("rep")[None]), me, mean_moment, *parts)
    return averaged.T, blended.T[None]


def solution(mesh):
    return jax.shard_map(
        body,
        mesh=mesh,
        in_specs=(
            P("rep", None, "shard"),
            P("rep", None, "shard"),
            P("rep", None, "shard", None),
            P("rep", None, None, "shard"),
            P("shard"),
        ),
        out_specs=(P(None, "shard"), P("rep", None, "shard")),
        check_vma=False,
    )
```
